256 devices in a mesh: seq: 64 (over x, z, core), grp: 4 (over y).
Axes of the slice: x: 4, y: 4, z: 8, core: 2. Of those that a mesh axis runs over, the one named last changes fastest.
Arguments:
- delta_codes: int32 [16, 16, 16384, 128], P('grp', None, 'seq'), may hold values from -63 to 63, as said below
- scale_index: int32 [16, 16, 1024], P('grp', None, 'seq'), may hold values from 0 to 15
- anchor_codes: int32 [16, 16, 128], P('grp'), may hold values from -8 to 7
- scale_table: float32 [16, 128], replicated, may hold values from 5e-05 to 0.0005
- anchor_scale: float32 [128], replicated, may hold values from 0.0001 to 0.001
Outputs:
- decode_cache: bfloat16 [4, 64, 16384, 128], P('grp', 'seq')
The draws below stay inside these ranges and needn't reach their ends.
Inputs may be any that keep to these rules, and one draw needn't show every extreme that they name: `delta_codes`: for every sequence, head and channel, the running sum of the codes from the sequence's first token lies in -32 .. 31 after every token, and in -2 .. 1 after the last token of each group of 16 tokens.
All inputs are finite; a program needn't handle non-finite values.
Results may differ from the reference program's by a relative error of at most 0.001.
Values may be sent and summed in bfloat16 or wider, within the bound.
A program may use at most 128 MiB of HBM per device.

```python
import math
import jax
import jax.numpy as jnp
from jax import lax

HEAD_DIM = 128
KV_HEADS = 16
GROUP_LEN = 16
LEVELS = 16
SEQS = 16
LENGTH = 16384
N_GRP = 4


def draw_delta_codes(key, part):
    running_key = jax.random.fold_in(key, 11)
    running = jax.random.randint(running_key, (SEQS, KV_HEADS, LENGTH, HEAD_DIM), -32, 32, dtype=jnp.int32)
    position = lax.broadcasted_iota(jnp.int32, (1, 1, LENGTH, 1), 2)
    group_end = position % GROUP_LEN == GROUP_LEN - 1
    running = jnp.where(group_end, jnp.remainder(running, 4) - 2, running)
    earlier = jnp.pad(running[:, :, :-1, :], ((0, 0), (0, 0), (1, 0), (0, 0)))
    return running - earlier


def plant(values, key, low, largest):
    dims = values.shape
    place = [jax.random.randint(jax.random.fold_in(key, axis), (), 0, dims[axis]) for axis in range(len(dims))]
    values = values.at[tuple(place)].set(low)
    longest = dims.index(max(dims))
    place[longest] = (place[longest] + 1) % dims[longest]
    return values.at[tuple(place)].set(largest)


def setup_inputs(seed: int = 0) -> dict:
    seeds = jax.random.split(jax.random.key(seed), 6)
    delta_codes = draw_delta_codes(jax.random.fold_in(seeds[5], 71), 0)
    scale_index = plant(jax.random.randint(seeds[1], (SEQS, KV_HEADS, LENGTH // GROUP_LEN), 0, LEVELS), jax.random.fold_in(seeds[1], 1), 0, LEVELS - 1).astype(jnp.int32)
    anchor_codes = plant(jax.random.randint(seeds[2], (SEQS, KV_HEADS, HEAD_DIM), -8, 8), jax.random.fold_in(seeds[2], 1), -8, 7).astype(jnp.int32)
    scale_table = jnp.clip(jnp.exp(jax.random.uniform(seeds[3], (LEVELS, HEAD_DIM), jnp.float32, math.log(4.999999873689376e-05), math.log(0.0005))), 4.999999873689376e-05, 0.0005)
    anchor_scale = jnp.clip(jnp.exp(jax.random.uniform(seeds[4], (HEAD_DIM,), jnp.float32, math.log(0.0001), math.log(0.001))), 0.0001, 0.001)
    return {"delta_codes": delta_codes, "scale_index": scale_index, "anchor_codes": anchor_codes, "scale_table": scale_table, "anchor_scale": anchor_scale}


def reference(delta_codes, scale_index, anchor_codes, scale_table, anchor_scale):
    def one_sequence(items):
        code_vals, scale_ids, anchors = items
        scales = scale_table[scale_ids]
        shaped = code_vals.astype(jnp.float32).reshape(KV_HEADS, LENGTH // GROUP_LEN, GROUP_LEN, HEAD_DIM)
        deltas = shaped * scales[:, :, None, :]
        summed = jnp.cumsum(deltas.reshape(KV_HEADS, LENGTH, HEAD_DIM), axis=1)
        anchor_vals = anchors.astype(jnp.float32) * anchor_scale
        return (summed + anchor_vals[:, None, :]).astype(jnp.bfloat16)

    rebuilt = lax.map(one_sequence, (delta_codes, scale_index, anchor_codes))
    arranged = rebuilt.reshape(SEQS, N_GRP, KV_HEADS // N_GRP, LENGTH, HEAD_DIM).transpose(1, 0, 2, 3, 4)
    return arranged.reshape(N_GRP, SEQS * (KV_HEADS // N_GRP), LENGTH, HEAD_DIM)
```

```python
import functools

import jax
import jax.numpy as jnp
from jax import lax
from jax.experimental import pallas as pl
from jax.experimental.pallas import tpu as pltpu
from jax.sharding import PartitionSpec as P

MESH = pl.DeviceIdType.MESH
NX, NY, NZ = 4, 4, 8
SLOTS = 4
ROUNDS = 16


def rounds_of(r):
    if r >= 14:
        return 0, 15 - r
    if r >= 12:
        return 4, r - 12
    return (r // 4 + 1) * (1 - 2 * (r % 2)), (r // 2) % 2


def exchange_kernel(
    codes, ids, anchors, anchor_scale, out, ids_out, anchor_out,
    stage, tri, summed, passed, id_src, id_pass, id_got,
    stage_sem, y_send, y_recv, f_send, f_recv, iy_send, iy_recv, if_send, if_recv, own_sem,
):
    s = lax.axis_index("seq")
    y = lax.axis_index("grp")
    core = s % 2
    z = (s // 2) % NZ
    x = s // (2 * NZ)
    here = z * 2 + core

    barrier = pltpu.get_barrier_semaphore()

    def greet(j, _):
        pl.semaphore_signal(barrier, inc=1, device_id=((s + j) % 64, y), device_id_type=MESH)
        return 0

    for k in range(1, NY):
        pl.semaphore_signal(barrier, inc=1, device_id=(s, (y + k) % NY), device_id_type=MESH)
    lax.fori_loop(1, 64, greet, 0)

    def fetch(n, slot):
        return pltpu.make_async_copy(
            codes.at[n // 4, pl.ds((n % 4) * 4, 4)], stage.at[slot], stage_sem.at[slot]
        )

    for n in range(SLOTS):
        fetch(n, n).start()

    levels = ids[...].astype(jnp.float32).reshape(64, 16)
    lane = lax.broadcasted_iota(jnp.int32, (16, 128), 1)
    entry = lax.broadcasted_iota(jnp.int32, (16, 128), 0)
    place = (lane == entry + (s % 8) * 16).astype(jnp.float32)
    spread = jnp.dot(levels, place, preferred_element_type=jnp.float32)
    for b in range(4):
        for k in range(16):
            id_src[k // 4, b * 4 + k % 4] = spread[b * 16 + k : b * 16 + k + 1, :]
    row_scale = anchor_scale[...]
    for h in range(4):
        id_src[h, 16] = anchors[here // 4, pl.ds(h * 4 + here % 4, 1), :].astype(jnp.float32) * row_scale

    row = lax.broadcasted_iota(jnp.int32, (256, 256), 0)
    col = lax.broadcasted_iota(jnp.int32, (256, 256), 1)
    tri[...] = ((row // 16 == col // 16) & (col <= row)).astype(jnp.float32).astype(jnp.bfloat16)

    def prefix(n, _):
        slot = n % SLOTS
        fetch(n, slot).wait()
        for q in range(0, 4, 2):
            pair = jnp.concatenate(
                [stage[slot, q].astype(jnp.float32), stage[slot, q + 1].astype(jnp.float32)], axis=1
            ).astype(jnp.bfloat16)
            sums = jnp.dot(tri[...], pair, preferred_element_type=jnp.float32).astype(jnp.bfloat16)
            summed[n % 4, (n // 4) * 4 + q] = sums[:, :128]
            summed[n % 4, (n // 4) * 4 + q + 1] = sums[:, 128:]

        @pl.when(n + SLOTS < 16)
        def _():
            fetch(n + SLOTS, slot).start()

        return 0

    lax.fori_loop(0, 16, prefix, 0)
    pl.semaphore_wait(barrier, 66)

    def target(r):
        dz, other = rounds_of(r)
        to_z = (z + dz + NZ) % NZ
        to_core = (core + other) % 2
        return to_z, to_core, to_z * 2 + to_core

    for k in range(1, NY):
        pltpu.make_async_remote_copy(
            src_ref=id_src.at[(y + k) % NY], dst_ref=id_pass.at[k - 1],
            send_sem=iy_send, recv_sem=iy_recv.at[k - 1],
            device_id=(s, (y + k) % NY), device_id_type=MESH,
        ).start()
    def send_y(r):
        _, _, m = target(r)
        for k in range(1, NY):
            pltpu.make_async_remote_copy(
                src_ref=summed.at[(y + k) % NY, m], dst_ref=passed.at[k - 1, r],
                send_sem=y_send, recv_sem=y_recv.at[k - 1, r],
                device_id=(s, (y + k) % NY), device_id_type=MESH,
            ).start()

    def send_final(r, k):
        to_z, to_core, m = target(r)
        to_x = (y - k + NX) % NX
        src = summed.at[y, m] if k == 0 else passed.at[k - 1, r]
        id_row = id_src.at[y, m] if k == 0 else id_pass.at[k - 1, m]

        def remote():
            where = ((to_x * NZ + to_z) * 2 + to_core, y)
            pltpu.make_async_remote_copy(
                src_ref=id_row, dst_ref=id_got.at[s], send_sem=if_send, recv_sem=if_recv,
                device_id=where, device_id_type=MESH,
            ).start()
            pltpu.make_async_remote_copy(
                src_ref=src, dst_ref=out.at[s], send_sem=f_send, recv_sem=f_recv,
                device_id=where, device_id_type=MESH,
            ).start()

        if r < 15:
            remote()
        else:
            pl.when(to_x != x)(remote)

            @pl.when(to_x == x)
            def _():
                id_got[s] = id_row[...]
                anchor_out[...] = (id_src[y, 16] if k == 0 else id_pass[k - 1, 16])
                pltpu.make_async_copy(src, out.at[s], own_sem).start()

    LEAD = 4
    for r in range(LEAD):
        send_y(r)
    for r in range(LEAD):
        send_final(r, 0)
    for r in range(LEAD, ROUNDS):
        send_y(r)
    for k in range(1, NY):
        pltpu.make_async_copy(id_pass.at[k - 1], id_pass.at[k - 1], iy_recv.at[k - 1]).wait()
    for r in range(ROUNDS):
        for k in range(1, NY):
            pltpu.make_async_copy(passed.at[k - 1, r], passed.at[k - 1, r], y_recv.at[k - 1, r]).wait()
            send_final(r, k)
        if r + LEAD < ROUNDS:
            send_final(r + LEAD, 0)

    pltpu.make_async_copy(id_got.at[pl.ds(0, 63)], id_got.at[pl.ds(0, 63)], if_recv).wait()
    for j in range(8):
        ids_out[pl.ds(j, 1), :] = functools.reduce(jnp.add, [id_got[j * 8 + i] for i in range(8)])
    pltpu.make_async_copy(out.at[0], out.at[0], own_sem).wait()
    pltpu.make_async_copy(passed, passed, y_send).wait()
    pltpu.make_async_copy(id_pass, id_pass, iy_send).wait()
    pltpu.make_async_copy(id_got.at[pl.ds(0, 63)], id_got.at[pl.ds(0, 63)], if_send).wait()
    pltpu.make_async_copy(out.at[pl.ds(0, 63)], out.at[pl.ds(0, 63)], f_send).wait()
    pltpu.make_async_copy(out.at[pl.ds(0, 63)], out.at[pl.ds(0, 63)], f_recv).wait()


def exchange(codes, ids, anchors, anchor_scale):
    vmem = pl.BlockSpec(memory_space=pltpu.VMEM)
    hbm = pl.BlockSpec(memory_space=pl.ANY)
    return pl.pallas_call(
        exchange_kernel,
        out_shape=(
            jax.ShapeDtypeStruct((64, 256, 128), jnp.bfloat16),
            jax.ShapeDtypeStruct((8, 128), jnp.float32),
            jax.ShapeDtypeStruct((1, 128), jnp.float32),
        ),
        in_specs=[hbm, vmem, vmem, vmem],
        out_specs=(hbm, vmem, vmem),
        scratch_shapes=[
            pltpu.VMEM((SLOTS, 4, 256, 128), jnp.int32),
            pltpu.VMEM((256, 256), jnp.bfloat16),
            pltpu.VMEM((4, 16, 256, 128), jnp.bfloat16),
            pltpu.VMEM((3, 16, 256, 128), jnp.bfloat16),
            pltpu.VMEM((4, 17, 1, 128), jnp.float32),
            pltpu.VMEM((3, 17, 1, 128), jnp.float32),
            pltpu.VMEM((64, 1, 128), jnp.float32),
            pltpu.SemaphoreType.DMA((SLOTS,)),
            pltpu.SemaphoreType.DMA,
            pltpu.SemaphoreType.DMA((3, ROUNDS)),
            pltpu.SemaphoreType.DMA,
            pltpu.SemaphoreType.DMA,
            pltpu.SemaphoreType.DMA,
            pltpu.SemaphoreType.DMA((3,)),
            pltpu.SemaphoreType.DMA,
            pltpu.SemaphoreType.DMA,
            pltpu.SemaphoreType.DMA,
        ],
        compiler_params=pltpu.CompilerParams(
            collective_id=0, has_side_effects=True, vmem_limit_bytes=40 * 2**20
        ),
        name="exchange",
    )(codes, ids, anchors, anchor_scale)


def rebuild_kernel(codes, ids, table, anchor, out, values, scales, carries, carry):
    step = pl.program_id(0)

    @pl.when(step == 0)
    def _():
        carry[...] = anchor[...]

    wanted = ids[pl.ds(step, 1), :]
    entry = lax.broadcasted_iota(jnp.int32, (16, 128), 0).astype(jnp.float32)
    onehot = (entry == wanted).astype(jnp.float32)
    scales[...] = lax.dot_general(
        onehot, table[...], (((0,), (0,)), ((), ())),
        precision=lax.Precision.HIGHEST, preferred_element_type=jnp.float32,
    )
    for j in range(128):
        block = codes[j // 16, pl.ds((j % 16) * 16, 16), :].astype(jnp.float32)
        values[pl.ds(j * 16, 16), :] = block * scales[pl.ds(j, 1), :]
    ends = values[pl.ds(15, 128, stride=16), :]
    row = lax.broadcasted_iota(jnp.int32, (128, 128), 0)
    col = lax.broadcasted_iota(jnp.int32, (128, 128), 1)
    strict = (col < row).astype(jnp.float32)
    before = jnp.dot(strict, ends, precision=lax.Precision.HIGHEST, preferred_element_type=jnp.float32)
    carries[...] = before + carry[...]
    carry[...] = carries[127:128, :] + ends[127:128, :]
    for j in range(128):
        block = values[pl.ds(j * 16, 16), :] + carries[pl.ds(j, 1), :]
        out[pl.ds(j * 16, 16), :] = block.astype(jnp.bfloat16)


def rebuild(codes, ids, table, anchor):
    return pl.pallas_call(
        rebuild_kernel,
        grid=(8,),
        out_shape=jax.ShapeDtypeStruct((16384, 128), jnp.bfloat16),
        in_specs=[
            pl.BlockSpec((8, 256, 128), lambda i: (i, 0, 0)),
            pl.BlockSpec((8, 128), lambda i: (0, 0)),
            pl.BlockSpec((16, 128), lambda i: (0, 0)),
            pl.BlockSpec((1, 128), lambda i: (0, 0)),
        ],
        out_specs=pl.BlockSpec((2048, 128), lambda i: (i, 0)),
        scratch_shapes=[
            pltpu.VMEM((2048, 128), jnp.float32),
            pltpu.VMEM((128, 128), jnp.float32),
            pltpu.VMEM((128, 128), jnp.float32),
            pltpu.VMEM((1, 128), jnp.float32),
        ],
        name="rebuild",
    )(codes, ids, table, anchor)


def on_device(delta_codes, scale_index, anchor_codes, scale_table, anchor_scale):
    codes, ids, anchor = exchange(delta_codes, scale_index, anchor_codes, anchor_scale.reshape(1, 128))
    return rebuild(codes, ids, scale_table, anchor).reshape(1, 1, 16384, 128)


def solution(mesh):
    placed = (P("grp", None, "seq", None), P("grp", None, "seq"), P("grp", None, None), P(), P())
    return jax.shard_map(
        on_device,
        mesh=mesh,
        in_specs=placed,
        out_specs=P("grp", "seq", None, None),
        check_vma=False,
    )
```

```python
import functools

import jax
import jax.numpy as jnp
from jax import lax
from jax.experimental import pallas as pl
from jax.experimental.pallas import tpu as pltpu
from jax.sharding import PartitionSpec as P

MESH = pl.DeviceIdType.MESH
NX, NY, NZ = 4, 4, 8
SLOTS = 4
ROUNDS = 16
LEAD = 2
PIECES = 8


ORDER = [(4, 0), (4, 1), (3, 0), (-3, 0), (3, 1), (-3, 1), (2, 0), (-2, 0), (2, 1), (-2, 1), (1, 0), (-1, 0), (1, 1), (-1, 1), (0, 1), (0, 0)]


def rounds_of(r):
    return ORDER[r]


def exchange_kernel(
    codes, ids_hbm, anchors_hbm, row_scale_hbm, table_hbm, grown, totals, anchor_out,
    stage, tri, blocks, landed, scales, ids, anchors, row_scale, table, id_rows, id_got,
    stage_sem, small_sem, y_send, y_recv, f_send, f_recv, iy_send, iy_recv, if_send, if_recv, own_sem,
):
    s = lax.axis_index("seq")
    y = lax.axis_index("grp")
    core = s % 2
    z = (s // 2) % NZ
    x = s // (2 * NZ)
    here = z * 2 + core

    def fetch(n, slot):
        return pltpu.make_async_copy(
            codes.at[n // 4, pl.ds((n % 4) * 4, 4)], stage.at[slot], stage_sem.at[slot]
        )

    for n in range(SLOTS):
        fetch(n, n).start()
    small = [
        pltpu.make_async_copy(ids_hbm, ids, small_sem.at[0]),
        pltpu.make_async_copy(anchors_hbm, anchors, small_sem.at[1]),
        pltpu.make_async_copy(row_scale_hbm, row_scale, small_sem.at[2]),
        pltpu.make_async_copy(table_hbm, table, small_sem.at[3]),
    ]
    for copy in small:
        copy.start()

    barrier = pltpu.get_barrier_semaphore()

    def greet(j, _):
        pl.semaphore_signal(barrier, inc=1, device_id=((s + j) % 64, y), device_id_type=MESH)
        return 0

    for k in range(1, NY):
        pl.semaphore_signal(barrier, inc=1, device_id=(s, (y + k) % NY), device_id_type=MESH)
    lax.fori_loop(1, 64, greet, 0)

    row = lax.broadcasted_iota(jnp.int32, (256, 256), 0)
    col = lax.broadcasted_iota(jnp.int32, (256, 256), 1)
    tri[...] = ((row // 16 == col // 16) & (col <= row)).astype(jnp.float32).astype(jnp.bfloat16)

    def prefix(n, _):
        slot = n % SLOTS
        fetch(n, slot).wait()
        for q in range(0, 4, 2):
            pair = jnp.concatenate(
                [stage[slot, q].astype(jnp.float32), stage[slot, q + 1].astype(jnp.float32)], axis=1
            ).astype(jnp.bfloat16)
            sums = jnp.dot(tri[...], pair, preferred_element_type=jnp.float32).astype(jnp.bfloat16)
            blocks[n % 4, (n // 4) * 4 + q] = sums[:, :128]
            blocks[n % 4, (n // 4) * 4 + q + 1] = sums[:, 128:]

        @pl.when(n + SLOTS < 16)
        def _():
            fetch(n + SLOTS, slot).start()

        return 0

    lax.fori_loop(0, 16, prefix, 0)

    for copy in small:
        copy.wait()
    levels = ids[...].astype(jnp.float32).reshape(64, 16)
    lane = lax.broadcasted_iota(jnp.int32, (16, 128), 1)
    entry = lax.broadcasted_iota(jnp.int32, (16, 128), 0)
    place = (lane == entry + (s % 8) * 16).astype(jnp.float32)
    spread = jnp.dot(levels, place, preferred_element_type=jnp.float32)
    for b in range(4):
        for k in range(16):
            id_rows[k // 4, b * 4 + k % 4] = spread[b * 16 + k : b * 16 + k + 1, :]
    for h in range(4):
        id_rows[h, 16] = (
            anchors[here // 4, pl.ds(h * 4 + here % 4, 1), :].astype(jnp.float32) * row_scale[...]
        )
    pl.semaphore_wait(barrier, 66)

    def target(r):
        dz, other = rounds_of(r)
        to_z = (z + dz + NZ) % NZ
        to_core = (core + other) % 2
        return to_z, to_core, to_z * 2 + to_core

    def slot_of(k):
        return jnp.where(k == 0, y, 3 + k)

    def pass_on(r):
        _, _, m = target(r)
        for k in (1, 3, 2):
            pltpu.make_async_remote_copy(
                src_ref=blocks.at[(y + k) % NY, m], dst_ref=blocks.at[3 + k, m],
                send_sem=y_send, recv_sem=y_recv.at[k - 1, r],
                device_id=(s, (y + k) % NY), device_id_type=MESH,
            ).start()

    def send(r, k, src, dst, send_sem, recv_sem):
        to_z, to_core, _ = target(r)
        to_x = (y - k + NX) % NX

        def remote():
            pltpu.make_async_remote_copy(
                src_ref=src, dst_ref=dst, send_sem=send_sem, recv_sem=recv_sem,
                device_id=((to_x * NZ + to_z) * 2 + to_core, y), device_id_type=MESH,
            ).start()

        if ORDER[r] == (0, 0):
            pl.when(to_x != x)(remote)
        else:
            remote()

    def send_block(r, k):
        send(r, k, blocks.at[slot_of(k), target(r)[2]], landed.at[s], f_send, f_recv.at[s])

    def send_ids(r, k):
        send(r, k, id_rows.at[slot_of(k), target(r)[2]], id_got.at[s], if_send, if_recv)

    for k in range(1, NY):
        pltpu.make_async_remote_copy(
            src_ref=id_rows.at[(y + k) % NY], dst_ref=id_rows.at[3 + k],
            send_sem=iy_send, recv_sem=iy_recv.at[k - 1],
            device_id=(s, (y + k) % NY), device_id_type=MESH,
        ).start()
    for r in range(LEAD):
        pass_on(r)
        send_block(r, 0)
    for r in range(LEAD, ROUNDS):
        pass_on(r)
    for k in range(1, NY):
        pltpu.make_async_copy(id_rows.at[3 + k], id_rows.at[3 + k], iy_recv.at[k - 1]).wait()
    for r in range(ROUNDS):
        for k in range(NY):
            send_ids(r, k)
    own = slot_of((y - x + NX) % NX)
    id_got[s] = id_rows[own, here]
    anchor_out[...] = id_rows[own, 16]
    for r in range(ROUNDS):
        for i in range(NX):
            k = (y - x - i - 2 * core - (1 if ORDER[r][0] < 0 else 0) + 12) % 4
            if r + LEAD < ROUNDS:
                pl.when(k == 0)(functools.partial(send_block, r + LEAD, 0))

            @pl.when(k != 0)
            def _():
                pltpu.make_async_copy(blocks.at[3 + k, 0], blocks.at[3 + k, 0], y_recv.at[k - 1, r]).wait()
                send_block(r, k)

    pltpu.make_async_copy(id_got.at[pl.ds(0, 63)], id_got.at[pl.ds(0, 63)], if_recv).wait()
    entry = lax.broadcasted_iota(jnp.int32, (16, 128), 0).astype(jnp.float32)
    for j in range(8):
        wanted = functools.reduce(jnp.add, [id_got[j * 8 + i] for i in range(8)])
        scales[pl.ds(j * 128, 128), :] = lax.dot_general(
            (entry == wanted).astype(jnp.float32), table[...], (((0,), (0,)), ((), ())),
            precision=lax.Precision.HIGHEST, preferred_element_type=jnp.float32,
        )

    def grow(block, at):
        run = jnp.zeros((1, 128), jnp.float32)
        for j in range(16):
            v = block[pl.ds(j * 16, 16), :].astype(jnp.float32) * scales[pl.ds(at * 16 + j, 1), :]
            grown[at, pl.ds(j * 16, 16), :] = v + run
            run = run + v[15:16, :]
        totals[pl.ds(at, 1), :] = run

    grow(blocks.at[own, here], s)

    for r in range(ROUNDS):
        dz, other = rounds_of(r)

        def take(j, _):
            from_x = (x + j) % NX
            at = (from_x * NZ + (z - dz + NZ) % NZ) * 2 + (core + other) % 2
            pltpu.make_async_copy(landed.at[at], landed.at[at], f_recv.at[at]).wait()
            grow(landed.at[at], at)
            return 0

        lax.fori_loop(1 if ORDER[r] == (0, 0) else 0, NX, take, 0)

    pltpu.make_async_copy(blocks.at[pl.ds(4, 3)], blocks.at[pl.ds(4, 3)], y_send).wait()
    pltpu.make_async_copy(id_rows.at[pl.ds(4, 3)], id_rows.at[pl.ds(4, 3)], iy_send).wait()
    pltpu.make_async_copy(id_got.at[pl.ds(0, 63)], id_got.at[pl.ds(0, 63)], if_send).wait()
    pltpu.make_async_copy(landed.at[pl.ds(0, 63)], landed.at[pl.ds(0, 63)], f_send).wait()


def exchange(codes, ids, anchors, anchor_scale, table):
    vmem = pl.BlockSpec(memory_space=pltpu.VMEM)
    hbm = pl.BlockSpec(memory_space=pltpu.HBM)
    return pl.pallas_call(
        exchange_kernel,
        out_shape=(
            jax.ShapeDtypeStruct((64, 256, 128), jnp.float32),
            jax.ShapeDtypeStruct((64, 128), jnp.float32),
            jax.ShapeDtypeStruct((1, 128), jnp.float32),
        ),
        in_specs=[hbm] * 5,
        out_specs=(vmem, vmem, vmem),
        scratch_shapes=[
            pltpu.VMEM((SLOTS, 4, 256, 128), jnp.int32),
            pltpu.VMEM((256, 256), jnp.bfloat16),
            pltpu.VMEM((7, 16, 256, 128), jnp.bfloat16),
            pltpu.VMEM((64, 256, 128), jnp.bfloat16),
            pltpu.VMEM((1024, 128), jnp.float32),
            pltpu.VMEM((4, 16, 16), jnp.int32),
            pltpu.VMEM((4, 16, 128), jnp.int32),
            pltpu.VMEM((1, 128), jnp.float32),
            pltpu.VMEM((16, 128), jnp.float32),
            pltpu.VMEM((7, 17, 1, 128), jnp.float32),
            pltpu.VMEM((64, 1, 128), jnp.float32),
            pltpu.SemaphoreType.DMA((SLOTS,)),
            pltpu.SemaphoreType.DMA((4,)),
            pltpu.SemaphoreType.DMA,
            pltpu.SemaphoreType.DMA((3, ROUNDS)),
            pltpu.SemaphoreType.DMA,
            pltpu.SemaphoreType.DMA((64,)),
            pltpu.SemaphoreType.DMA,
            pltpu.SemaphoreType.DMA((3,)),
            pltpu.SemaphoreType.DMA,
            pltpu.SemaphoreType.DMA,
            pltpu.SemaphoreType.DMA,
        ],
        compiler_params=pltpu.CompilerParams(
            collective_id=0, has_side_effects=True, vmem_limit_bytes=18 * 2**20
        ),
        name="exchange",
    )(*[pltpu.with_memory_space_constraint(a, pltpu.HBM) for a in (codes, ids, anchors, anchor_scale, table)])


def finish_kernel(grown, totals, anchor, out, rounded, sem):
    carry = anchor[...]
    copies = []
    for n in range(PIECES):
        blocks = 64 // PIECES

        def add(i, carry):
            at = n * blocks + i
            rounded[at] = (grown[at] + carry).astype(jnp.bfloat16)
            return carry + totals[pl.ds(at, 1), :]

        carry = lax.fori_loop(0, blocks, add, carry)
        piece = pl.ds(n * blocks, blocks)
        copies.append(pltpu.make_async_copy(rounded.at[piece], out.at[piece], sem.at[n]))
        copies[-1].start()
    for copy in copies:
        copy.wait()


def finish(grown, totals, anchor):
    vmem = pl.BlockSpec(memory_space=pltpu.VMEM)
    return pl.pallas_call(
        finish_kernel,
        out_shape=jax.ShapeDtypeStruct((64, 256, 128), jnp.bfloat16),
        in_specs=[vmem, vmem, vmem],
        out_specs=pl.BlockSpec(memory_space=pltpu.HBM),
        scratch_shapes=[
            pltpu.VMEM((64, 256, 128), jnp.bfloat16),
            pltpu.SemaphoreType.DMA((PIECES,)),
        ],
        compiler_params=pltpu.CompilerParams(vmem_limit_bytes=6 * 2**20),
        name="finish",
    )(grown, totals, anchor)


def on_device(delta_codes, scale_index, anchor_codes, scale_table, anchor_scale):
    grown, totals, anchor = exchange(
        delta_codes, scale_index, anchor_codes, anchor_scale.reshape(1, 128), scale_table
    )
    return finish(grown, totals, anchor).reshape(1, 1, 16384, 128)


def solution(mesh):
    placed = (P("grp", None, "seq", None), P("grp", None, "seq"), P("grp", None, None), P(), P())
    return jax.shard_map(
        on_device,
        mesh=mesh,
        in_specs=placed,
        out_specs=P("grp", "seq", None, None),
        check_vma=False,
    )
```

```python
import functools

import jax
import jax.numpy as jnp
from jax import lax
from jax.experimental import pallas as pl
from jax.experimental.pallas import tpu as pltpu
from jax.sharding import PartitionSpec as P

MESH = pl.DeviceIdType.MESH
NX, NY, NZ = 4, 4, 8
SLOTS = 4
ROUNDS = 16
LEAD = 2
AHEAD = 2
IDS_AT = 3
PIECES = 8


ORDER = [(4, 0), (4, 1), (3, 0), (-3, 0), (3, 1), (-3, 1), (2, 0), (-2, 0), (2, 1), (-2, 1), (1, 0), (-1, 0), (1, 1), (-1, 1), (0, 1), (0, 0)]


def rounds_of(r):
    return ORDER[r]


def exchange_kernel(
    codes, ids_hbm, anchors_hbm, row_scale_hbm, table_hbm, grown, totals, anchor_out,
    stage, tri, blocks, landed, scales, ids, anchors, row_scale, table, id_rows, id_got,
    stage_sem, small_sem, y_send, y_recv, f_send, f_recv, iy_send, iy_recv, if_send, if_recv, own_sem,
):
    s = lax.axis_index("seq")
    y = lax.axis_index("grp")
    core = s % 2
    z = (s // 2) % NZ
    x = s // (2 * NZ)
    here = z * 2 + core

    def target(r):
        dz, other = rounds_of(r)
        to_z = (z + dz + NZ) % NZ
        to_core = (core + other) % 2
        return to_z, to_core, to_z * 2 + to_core

    def fetch(r):
        m = target(r)[2]
        return pltpu.make_async_copy(
            codes.at[m // 4, :, m % 4], stage.at[r % SLOTS], stage_sem.at[r % SLOTS]
        )

    for r in range(SLOTS):
        fetch(r).start()
    small = [
        pltpu.make_async_copy(ids_hbm, ids, small_sem.at[0]),
        pltpu.make_async_copy(anchors_hbm, anchors, small_sem.at[1]),
        pltpu.make_async_copy(row_scale_hbm, row_scale, small_sem.at[2]),
        pltpu.make_async_copy(table_hbm, table, small_sem.at[3]),
    ]
    for copy in small:
        copy.start()

    barrier = pltpu.get_barrier_semaphore()

    def greet(j, _):
        pl.semaphore_signal(barrier, inc=1, device_id=((s + j) % 64, y), device_id_type=MESH)
        return 0

    for k in range(1, NY):
        pl.semaphore_signal(barrier, inc=1, device_id=(s, (y + k) % NY), device_id_type=MESH)
    lax.fori_loop(1, 64, greet, 0)

    row = lax.broadcasted_iota(jnp.int32, (256, 256), 0)
    col = lax.broadcasted_iota(jnp.int32, (256, 256), 1)
    tri[...] = ((row // 16 == col // 16) & (col <= row)).astype(jnp.float32).astype(jnp.bfloat16)

    def prefix(r):
        m = target(r)[2]
        fetch(r).wait()
        for h in range(0, 4, 2):
            pair = jnp.concatenate(
                [stage[r % SLOTS, h].astype(jnp.float32), stage[r % SLOTS, h + 1].astype(jnp.float32)], axis=1
            ).astype(jnp.bfloat16)
            sums = jnp.dot(tri[...], pair, preferred_element_type=jnp.float32).astype(jnp.bfloat16)
            blocks[h, m] = sums[:, :128]
            blocks[h + 1, m] = sums[:, 128:]
        if r + SLOTS < ROUNDS:
            fetch(r + SLOTS).start()

    def write_ids():
        for copy in small:
            copy.wait()
        levels = ids[...].astype(jnp.float32).reshape(64, 16)
        lane = lax.broadcasted_iota(jnp.int32, (16, 128), 1)
        entry = lax.broadcasted_iota(jnp.int32, (16, 128), 0)
        place = (lane == entry + (s % 8) * 16).astype(jnp.float32)
        spread = jnp.dot(levels, place, preferred_element_type=jnp.float32)
        for b in range(4):
            for k in range(16):
                id_rows[k // 4, b * 4 + k % 4] = spread[b * 16 + k : b * 16 + k + 1, :]
        for h in range(4):
            id_rows[h, 16] = (
                anchors[here // 4, pl.ds(h * 4 + here % 4, 1), :].astype(jnp.float32) * row_scale[...]
            )

    def slot_of(k):
        return jnp.where(k == 0, y, 3 + k)

    def pass_on(r):
        _, _, m = target(r)
        for k in (1, 3, 2):
            pltpu.make_async_remote_copy(
                src_ref=blocks.at[(y + k) % NY, m], dst_ref=blocks.at[3 + k, m],
                send_sem=y_send, recv_sem=y_recv.at[k - 1, r],
                device_id=(s, (y + k) % NY), device_id_type=MESH,
            ).start()

    def send(r, k, src, dst, send_sem, recv_sem):
        to_z, to_core, _ = target(r)
        to_x = (y - k + NX) % NX

        def remote():
            pltpu.make_async_remote_copy(
                src_ref=src, dst_ref=dst, send_sem=send_sem, recv_sem=recv_sem,
                device_id=((to_x * NZ + to_z) * 2 + to_core, y), device_id_type=MESH,
            ).start()

        if ORDER[r] == (0, 0):
            pl.when(to_x != x)(remote)
        else:
            remote()

    def send_block(r, k):
        send(r, k, blocks.at[slot_of(k), target(r)[2]], landed.at[s], f_send, f_recv.at[s])

    def send_ids(r, k):
        send(r, k, id_rows.at[slot_of(k), target(r)[2]], id_got.at[s], if_send, if_recv)

    for r in range(AHEAD):
        prefix(r)
    pl.semaphore_wait(barrier, 66)
    for r in range(ROUNDS):
        if r + AHEAD < ROUNDS:
            prefix(r + AHEAD)
        pass_on(r)
        if r < LEAD:
            send_block(r, 0)
        if r == 2:
            for k in range(1, NY):
                pltpu.make_async_remote_copy(
                    src_ref=id_rows.at[(y + k) % NY], dst_ref=id_rows.at[3 + k],
                    send_sem=iy_send, recv_sem=iy_recv.at[k - 1],
                    device_id=(s, (y + k) % NY), device_id_type=MESH,
                ).start()
        if r == 1:
            write_ids()
    own = slot_of((y - x + NX) % NX)
    for r in range(ROUNDS):
        for i in range(NX):
            k = (y - x - i - 2 * core - (1 if ORDER[r][0] < 0 else 0) + 12) % 4
            if r >= LEAD:
                pl.when(k == 0)(functools.partial(send_block, r, 0))

            @pl.when(k != 0)
            def _():
                pltpu.make_async_copy(blocks.at[3 + k, 0], blocks.at[3 + k, 0], y_recv.at[k - 1, r]).wait()
                send_block(r, k)

        if r == IDS_AT:
            for k in range(1, NY):
                pltpu.make_async_copy(id_rows.at[3 + k], id_rows.at[3 + k], iy_recv.at[k - 1]).wait()
            for n in range(ROUNDS):
                for k in range(NY):
                    send_ids(n, k)
            id_got[s] = id_rows[own, here]
            anchor_out[...] = id_rows[own, 16]

    pltpu.make_async_copy(id_got.at[pl.ds(0, 63)], id_got.at[pl.ds(0, 63)], if_recv).wait()
    entry = lax.broadcasted_iota(jnp.int32, (16, 128), 0).astype(jnp.float32)
    for j in range(8):
        wanted = functools.reduce(jnp.add, [id_got[j * 8 + i] for i in range(8)])
        scales[pl.ds(j * 128, 128), :] = lax.dot_general(
            (entry == wanted).astype(jnp.float32), table[...], (((0,), (0,)), ((), ())),
            precision=lax.Precision.HIGHEST, preferred_element_type=jnp.float32,
        )

    def grow(block, at):
        run = jnp.zeros((1, 128), jnp.float32)
        for j in range(16):
            v = block[pl.ds(j * 16, 16), :].astype(jnp.float32) * scales[pl.ds(at * 16 + j, 1), :]
            grown[at, pl.ds(j * 16, 16), :] = v + run
            run = run + v[15:16, :]
        totals[pl.ds(at, 1), :] = run

    grow(blocks.at[own, here], s)

    for r in range(ROUNDS):
        dz, other = rounds_of(r)

        def take(j, _):
            from_x = (x + j) % NX
            at = (from_x * NZ + (z - dz + NZ) % NZ) * 2 + (core + other) % 2
            pltpu.make_async_copy(landed.at[at], landed.at[at], f_recv.at[at]).wait()
            grow(landed.at[at], at)
            return 0

        lax.fori_loop(1 if ORDER[r] == (0, 0) else 0, NX, take, 0)

    pltpu.make_async_copy(blocks.at[pl.ds(4, 3)], blocks.at[pl.ds(4, 3)], y_send).wait()
    pltpu.make_async_copy(id_rows.at[pl.ds(4, 3)], id_rows.at[pl.ds(4, 3)], iy_send).wait()
    pltpu.make_async_copy(id_got.at[pl.ds(0, 63)], id_got.at[pl.ds(0, 63)], if_send).wait()
    pltpu.make_async_copy(landed.at[pl.ds(0, 63)], landed.at[pl.ds(0, 63)], f_send).wait()


def exchange(codes, ids, anchors, anchor_scale, table):
    vmem = pl.BlockSpec(memory_space=pltpu.VMEM)
    hbm = pl.BlockSpec(memory_space=pltpu.HBM)
    return pl.pallas_call(
        exchange_kernel,
        out_shape=(
            jax.ShapeDtypeStruct((64, 256, 128), jnp.float32),
            jax.ShapeDtypeStruct((64, 128), jnp.float32),
            jax.ShapeDtypeStruct((1, 128), jnp.float32),
        ),
        in_specs=[hbm] * 5,
        out_specs=(vmem, vmem, vmem),
        scratch_shapes=[
            pltpu.VMEM((SLOTS, 4, 256, 128), jnp.int32),
            pltpu.VMEM((256, 256), jnp.bfloat16),
            pltpu.VMEM((7, 16, 256, 128), jnp.bfloat16),
            pltpu.VMEM((64, 256, 128), jnp.bfloat16),
            pltpu.VMEM((1024, 128), jnp.float32),
            pltpu.VMEM((4, 16, 16), jnp.int32),
            pltpu.VMEM((4, 16, 128), jnp.int32),
            pltpu.VMEM((1, 128), jnp.float32),
            pltpu.VMEM((16, 128), jnp.float32),
            pltpu.VMEM((7, 17, 1, 128), jnp.float32),
            pltpu.VMEM((64, 1, 128), jnp.float32),
            pltpu.SemaphoreType.DMA((SLOTS,)),
            pltpu.SemaphoreType.DMA((4,)),
            pltpu.SemaphoreType.DMA,
            pltpu.SemaphoreType.DMA((3, ROUNDS)),
            pltpu.SemaphoreType.DMA,
            pltpu.SemaphoreType.DMA((64,)),
            pltpu.SemaphoreType.DMA,
            pltpu.SemaphoreType.DMA((3,)),
            pltpu.SemaphoreType.DMA,
            pltpu.SemaphoreType.DMA,
            pltpu.SemaphoreType.DMA,
        ],
        compiler_params=pltpu.CompilerParams(
            collective_id=0, has_side_effects=True, vmem_limit_bytes=18 * 2**20
        ),
        name="exchange",
    )(*[pltpu.with_memory_space_constraint(a, pltpu.HBM) for a in (codes, ids, anchors, anchor_scale, table)])


def finish_kernel(grown, totals, anchor, out, rounded, sem):
    carry = anchor[...]
    copies = []
    for n in range(PIECES):
        blocks = 64 // PIECES

        def add(i, carry):
            at = n * blocks + i
            rounded[at] = (grown[at] + carry).astype(jnp.bfloat16)
            return carry + totals[pl.ds(at, 1), :]

        carry = lax.fori_loop(0, blocks, add, carry)
        piece = pl.ds(n * blocks, blocks)
        copies.append(pltpu.make_async_copy(rounded.at[piece], out.at[piece], sem.at[n]))
        copies[-1].start()
    for copy in copies:
        copy.wait()


def finish(grown, totals, anchor):
    vmem = pl.BlockSpec(memory_space=pltpu.VMEM)
    return pl.pallas_call(
        finish_kernel,
        out_shape=jax.ShapeDtypeStruct((64, 256, 128), jnp.bfloat16),
        in_specs=[vmem, vmem, vmem],
        out_specs=pl.BlockSpec(memory_space=pltpu.HBM),
        scratch_shapes=[
            pltpu.VMEM((64, 256, 128), jnp.bfloat16),
            pltpu.SemaphoreType.DMA((PIECES,)),
        ],
        compiler_params=pltpu.CompilerParams(vmem_limit_bytes=6 * 2**20),
        name="finish",
    )(grown, totals, anchor)


def on_device(delta_codes, scale_index, anchor_codes, scale_table, anchor_scale):
    grown, totals, anchor = exchange(
        delta_codes.reshape(4, 4, 4, 256, 128), scale_index, anchor_codes, anchor_scale.reshape(1, 128), scale_table
    )
    return finish(grown, totals, anchor).reshape(1, 1, 16384, 128)


def solution(mesh):
    placed = (P("grp", None, "seq", None), P("grp", None, "seq"), P("grp", None, None), P(), P())
    return jax.shard_map(
        on_device,
        mesh=mesh,
        in_specs=placed,
        out_specs=P("grp", "seq", None, None),
        check_vma=False,
    )
```

```python
import functools

import jax
import jax.numpy as jnp
from jax import lax
from jax.experimental import pallas as pl
from jax.experimental.pallas import tpu as pltpu
from jax.sharding import PartitionSpec as P

MESH = pl.DeviceIdType.MESH
NX, NY, NZ = 4, 4, 8
SLOTS = 4
ROUNDS = 16
LEAD = 2
AHEAD = 2
IDS_AT = 3
PIECES = 8


ORDER = [(4, 0), (4, 1), (3, 0), (-3, 0), (3, 1), (-3, 1), (2, 0), (-2, 0), (2, 1), (-2, 1), (1, 0), (-1, 0), (1, 1), (-1, 1), (0, 1), (0, 0)]


def rounds_of(r):
    return ORDER[r]


def exchange_kernel(
    codes, ids_hbm, anchors_hbm, row_scale_hbm, table_hbm, grown, totals, anchor_out,
    stage, tri, blocks, landed, scales, ids, anchors, row_scale, table, id_rows, id_got,
    stage_sem, small_sem, y_send, y_recv, f_send, f_recv, iy_send, iy_recv, if_send, if_recv, own_sem,
):
    s = lax.axis_index("seq")
    y = lax.axis_index("grp")
    core = s % 2
    z = (s // 2) % NZ
    x = s // (2 * NZ)
    here = z * 2 + core

    def target(r):
        dz, other = rounds_of(r)
        to_z = (z + dz + NZ) % NZ
        to_core = (core + other) % 2
        return to_z, to_core, to_z * 2 + to_core

    def fetch(r):
        m = target(r)[2]
        return pltpu.make_async_copy(
            codes.at[m // 4, :, m % 4], stage.at[r % SLOTS], stage_sem.at[r % SLOTS]
        )

    for r in range(AHEAD):
        fetch(r).start()
    barrier = pltpu.get_barrier_semaphore()

    def greet(j, _):
        pl.semaphore_signal(barrier, inc=1, device_id=((s + j) % 64, y), device_id_type=MESH)
        return 0

    lax.fori_loop(24, 64, greet, 0)
    lax.fori_loop(1, 24, greet, 0)
    for k in range(1, NY):
        pl.semaphore_signal(barrier, inc=1, device_id=(s, (y + k) % NY), device_id_type=MESH)
    for r in range(AHEAD, SLOTS):
        fetch(r).start()
    small = [
        pltpu.make_async_copy(ids_hbm, ids, small_sem.at[0]),
        pltpu.make_async_copy(anchors_hbm, anchors, small_sem.at[1]),
        pltpu.make_async_copy(row_scale_hbm, row_scale, small_sem.at[2]),
        pltpu.make_async_copy(table_hbm, table, small_sem.at[3]),
    ]
    for copy in small:
        copy.start()

    row = lax.broadcasted_iota(jnp.int32, (256, 256), 0)
    col = lax.broadcasted_iota(jnp.int32, (256, 256), 1)
    tri[...] = ((row // 16 == col // 16) & (col <= row)).astype(jnp.float32).astype(jnp.bfloat16)

    def prefix(r):
        m = target(r)[2]
        fetch(r).wait()
        for h in range(0, 4, 2):
            pair = jnp.concatenate(
                [stage[r % SLOTS, h].astype(jnp.float32), stage[r % SLOTS, h + 1].astype(jnp.float32)], axis=1
            ).astype(jnp.bfloat16)
            sums = jnp.dot(tri[...], pair, preferred_element_type=jnp.float32).astype(jnp.bfloat16)
            blocks[h, m] = sums[:, :128]
            blocks[h + 1, m] = sums[:, 128:]
        if r + SLOTS < ROUNDS:
            fetch(r + SLOTS).start()

    def write_ids():
        for copy in small:
            copy.wait()
        levels = ids[...].astype(jnp.float32).reshape(64, 16)
        lane = lax.broadcasted_iota(jnp.int32, (16, 128), 1)
        entry = lax.broadcasted_iota(jnp.int32, (16, 128), 0)
        place = (lane == entry + (s % 8) * 16).astype(jnp.float32)
        spread = jnp.dot(levels, place, preferred_element_type=jnp.float32)
        for b in range(4):
            for k in range(16):
                id_rows[k // 4, b * 4 + k % 4] = spread[b * 16 + k : b * 16 + k + 1, :]
        for h in range(4):
            id_rows[h, 16] = (
                anchors[here // 4, pl.ds(h * 4 + here % 4, 1), :].astype(jnp.float32) * row_scale[...]
            )

    def slot_of(k):
        return jnp.where(k == 0, y, 3 + k)

    def pass_on(r):
        _, _, m = target(r)
        for k in (1, 3, 2):
            pltpu.make_async_remote_copy(
                src_ref=blocks.at[(y + k) % NY, m], dst_ref=blocks.at[3 + k, m],
                send_sem=y_send, recv_sem=y_recv.at[k - 1, r],
                device_id=(s, (y + k) % NY), device_id_type=MESH,
            ).start()

    def send(r, k, src, dst, send_sem, recv_sem):
        to_z, to_core, _ = target(r)
        to_x = (y - k + NX) % NX

        def remote():
            pltpu.make_async_remote_copy(
                src_ref=src, dst_ref=dst, send_sem=send_sem, recv_sem=recv_sem,
                device_id=((to_x * NZ + to_z) * 2 + to_core, y), device_id_type=MESH,
            ).start()

        if ORDER[r] == (0, 0):
            pl.when(to_x != x)(remote)
        else:
            remote()

    def send_block(r, k):
        send(r, k, blocks.at[slot_of(k), target(r)[2]], landed.at[s], f_send, f_recv.at[s])

    def send_ids(r, k):
        send(r, k, id_rows.at[slot_of(k), target(r)[2]], id_got.at[s], if_send, if_recv)

    for r in range(AHEAD):
        prefix(r)
    pl.semaphore_wait(barrier, 66)
    for r in range(ROUNDS):
        if r + AHEAD < ROUNDS:
            prefix(r + AHEAD)
        pass_on(r)
        if r < LEAD:
            send_block(r, 0)
        if r == 2:
            for k in range(1, NY):
                pltpu.make_async_remote_copy(
                    src_ref=id_rows.at[(y + k) % NY], dst_ref=id_rows.at[3 + k],
                    send_sem=iy_send, recv_sem=iy_recv.at[k - 1],
                    device_id=(s, (y + k) % NY), device_id_type=MESH,
                ).start()
        if r == 1:
            write_ids()
    own = slot_of((y - x + NX) % NX)
    for r in range(ROUNDS):
        for i in range(NX):
            k = (y - x - i - core - (2 if ORDER[r][0] < 0 else 0) + 12) % 4
            if r >= LEAD:
                pl.when(k == 0)(functools.partial(send_block, r, 0))

            @pl.when(k != 0)
            def _():
                pltpu.make_async_copy(blocks.at[3 + k, 0], blocks.at[3 + k, 0], y_recv.at[k - 1, r]).wait()
                send_block(r, k)

        if r == IDS_AT:
            for k in range(1, NY):
                pltpu.make_async_copy(id_rows.at[3 + k], id_rows.at[3 + k], iy_recv.at[k - 1]).wait()
            for n in range(ROUNDS):
                for k in range(NY):
                    send_ids(n, k)
            id_got[s] = id_rows[own, here]
            anchor_out[...] = id_rows[own, 16]

    pltpu.make_async_copy(id_got.at[pl.ds(0, 63)], id_got.at[pl.ds(0, 63)], if_recv).wait()
    entry = lax.broadcasted_iota(jnp.int32, (16, 128), 0).astype(jnp.float32)
    for j in range(8):
        wanted = functools.reduce(jnp.add, [id_got[j * 8 + i] for i in range(8)])
        scales[pl.ds(j * 128, 128), :] = lax.dot_general(
            (entry == wanted).astype(jnp.float32), table[...], (((0,), (0,)), ((), ())),
            precision=lax.Precision.HIGHEST, preferred_element_type=jnp.float32,
        )

    def grow(block, at):
        run = jnp.zeros((1, 128), jnp.float32)
        for j in range(16):
            v = block[pl.ds(j * 16, 16), :].astype(jnp.float32) * scales[pl.ds(at * 16 + j, 1), :]
            grown[at, pl.ds(j * 16, 16), :] = v + run
            run = run + v[15:16, :]
        totals[pl.ds(at, 1), :] = run

    grow(blocks.at[own, here], s)

    for r in range(ROUNDS):
        dz, other = rounds_of(r)

        def take(j, _):
            from_x = (x + j) % NX
            at = (from_x * NZ + (z - dz + NZ) % NZ) * 2 + (core + other) % 2
            pltpu.make_async_copy(landed.at[at], landed.at[at], f_recv.at[at]).wait()
            grow(landed.at[at], at)
            return 0

        lax.fori_loop(1 if ORDER[r] == (0, 0) else 0, NX, take, 0)

    pltpu.make_async_copy(blocks.at[pl.ds(4, 3)], blocks.at[pl.ds(4, 3)], y_send).wait()
    pltpu.make_async_copy(id_rows.at[pl.ds(4, 3)], id_rows.at[pl.ds(4, 3)], iy_send).wait()
    pltpu.make_async_copy(id_got.at[pl.ds(0, 63)], id_got.at[pl.ds(0, 63)], if_send).wait()
    pltpu.make_async_copy(landed.at[pl.ds(0, 63)], landed.at[pl.ds(0, 63)], f_send).wait()


def exchange(codes, ids, anchors, anchor_scale, table):
    vmem = pl.BlockSpec(memory_space=pltpu.VMEM)
    hbm = pl.BlockSpec(memory_space=pltpu.HBM)
    return pl.pallas_call(
        exchange_kernel,
        out_shape=(
            jax.ShapeDtypeStruct((64, 256, 128), jnp.float32),
            jax.ShapeDtypeStruct((64, 128), jnp.float32),
            jax.ShapeDtypeStruct((1, 128), jnp.float32),
        ),
        in_specs=[hbm] * 5,
        out_specs=(vmem, vmem, vmem),
        scratch_shapes=[
            pltpu.VMEM((SLOTS, 4, 256, 128), jnp.int32),
            pltpu.VMEM((256, 256), jnp.bfloat16),
            pltpu.VMEM((7, 16, 256, 128), jnp.bfloat16),
            pltpu.VMEM((64, 256, 128), jnp.bfloat16),
            pltpu.VMEM((1024, 128), jnp.float32),
            pltpu.VMEM((4, 16, 16), jnp.int32),
            pltpu.VMEM((4, 16, 128), jnp.int32),
            pltpu.VMEM((1, 128), jnp.float32),
            pltpu.VMEM((16, 128), jnp.float32),
            pltpu.VMEM((7, 17, 1, 128), jnp.float32),
            pltpu.VMEM((64, 1, 128), jnp.float32),
            pltpu.SemaphoreType.DMA((SLOTS,)),
            pltpu.SemaphoreType.DMA((4,)),
            pltpu.SemaphoreType.DMA,
            pltpu.SemaphoreType.DMA((3, ROUNDS)),
            pltpu.SemaphoreType.DMA,
            pltpu.SemaphoreType.DMA((64,)),
            pltpu.SemaphoreType.DMA,
            pltpu.SemaphoreType.DMA((3,)),
            pltpu.SemaphoreType.DMA,
            pltpu.SemaphoreType.DMA,
            pltpu.SemaphoreType.DMA,
        ],
        compiler_params=pltpu.CompilerParams(
            collective_id=0, has_side_effects=True, vmem_limit_bytes=18 * 2**20
        ),
        name="exchange",
    )(*[pltpu.with_memory_space_constraint(a, pltpu.HBM) for a in (codes, ids, anchors, anchor_scale, table)])


def finish_kernel(grown, totals, anchor, out, rounded, sem):
    carry = anchor[...]
    copies = []
    for n in range(PIECES):
        blocks = 64 // PIECES

        def add(i, carry):
            at = n * blocks + i
            rounded[at] = (grown[at] + carry).astype(jnp.bfloat16)
            return carry + totals[pl.ds(at, 1), :]

        carry = lax.fori_loop(0, blocks, add, carry)
        piece = pl.ds(n * blocks, blocks)
        copies.append(pltpu.make_async_copy(rounded.at[piece], out.at[piece], sem.at[n]))
        copies[-1].start()
    for copy in copies:
        copy.wait()


def finish(grown, totals, anchor):
    vmem = pl.BlockSpec(memory_space=pltpu.VMEM)
    return pl.pallas_call(
        finish_kernel,
        out_shape=jax.ShapeDtypeStruct((64, 256, 128), jnp.bfloat16),
        in_specs=[vmem, vmem, vmem],
        out_specs=pl.BlockSpec(memory_space=pltpu.HBM),
        scratch_shapes=[
            pltpu.VMEM((64, 256, 128), jnp.bfloat16),
            pltpu.SemaphoreType.DMA((PIECES,)),
        ],
        compiler_params=pltpu.CompilerParams(vmem_limit_bytes=6 * 2**20),
        name="finish",
    )(grown, totals, anchor)


def on_device(delta_codes, scale_index, anchor_codes, scale_table, anchor_scale):
    grown, totals, anchor = exchange(
        delta_codes.reshape(4, 4, 4, 256, 128), scale_index, anchor_codes, anchor_scale.reshape(1, 128), scale_table
    )
    return finish(grown, totals, anchor).reshape(1, 1, 16384, 128)


def solution(mesh):
    placed = (P("grp", None, "seq", None), P("grp", None, "seq"), P("grp", None, None), P(), P())
    return jax.shard_map(
        on_device,
        mesh=mesh,
        in_specs=placed,
        out_specs=P("grp", "seq", None, None),
        check_vma=False,
    )
```
